256 devices in a mesh: dp: 32 (over z, y_lo, core), expert: 8 (over y_hi, x).
Axes of the slice: x: 4, y: 4 (y_hi: 2, y_lo: 2; y = y_hi * 2 + y_lo), z: 8, core: 2. Of those that a mesh axis runs over, the one named last changes fastest.
Arguments:
- tokens: bfloat16 [2048, 6144], P(('dp', 'expert')), may hold values from -6 to 6
- router_now: float32 [6144, 8], P('dp'), may hold values from -0.078125 to 0.078125
- router_next: float32 [6144, 8], P('dp'), may hold values from -0.078125 to 0.078125
- w_gate: bfloat16 [8, 6144, 8192], P('expert', None, 'dp'), may hold values from -0.078125 to 0.078125
- w_up: bfloat16 [8, 6144, 8192], P('expert', None, 'dp'), may hold values from -0.078125 to 0.078125
- w_down: bfloat16 [8, 8192, 6144], P('expert', 'dp'), may hold values from -0.0625 to 0.0625
- expert_ids: int32 [2048, 2], P(('dp', 'expert')), may hold values from 0 to 7, all different within a row; in each aligned block of 8 rows (0 to 7, 8 to 15, ...) at most 4 rows name the same one
- next_ids: int32 [2048, 2], P(('dp', 'expert')), may hold values from 0 to 7, all different within a row
Outputs:
- layer_out: bfloat16 [2048, 6144], P(('dp', 'expert'))
- next_logits: float32 [2048, 8], P(('dp', 'expert'))
- next_weights: float32 [2048, 2], P(('dp', 'expert'))
The draws below stay inside these ranges and needn't reach their ends.
Inputs may be any that keep to these rules, and one draw needn't show every extreme that they name: `expert_ids`: each row names 2 different experts. Among the 8 rows of one device no expert is named by more than 4 rows, and on some devices one expert is named by exactly 4 rows. `next_ids`: each row names 2 different experts.
All inputs are finite; a program needn't handle non-finite values.
Results may differ from the reference program's by a relative error of at most 0.013.
Values may be sent and summed in bfloat16 or wider, within the bound.
No kernel may reach another device: no remote copies, remote signals or barrier semaphores. Data moves between devices by JAX's collectives and lax.ppermute only.
A program may use at most 128 MiB of HBM per device.

```python
import math
import jax
import jax.numpy as jnp
import numpy as np
from jax import lax

D = 6144
FF = 8192
EXPERTS = 8
TOP = 2
TOK_DEV = 8
CAP = 4
TOKENS = 2048


def levels(rng, extent, shards, low, top_value):
    gain, own = 1.0, jax.random.fold_in(rng, 6)
    for position, parts in shards:
        heights = jnp.exp(jax.random.uniform(jax.random.fold_in(own, position), (parts,), jnp.float32, low / len(shards), top_value / len(shards)))
        gain = gain * jnp.repeat(heights, extent[position] // parts).reshape([-1 if axis == position else 1 for axis in range(len(extent))])
    return gain


def picks_of(rng, rows, amount, top, lift):
    order = jax.random.permutation(jax.random.fold_in(rng, 1), amount)
    favour = order
    for power in range(3):
        favour = favour * favour // amount
    favour = favour * lift // amount
    tickets = jax.random.randint(jax.random.fold_in(rng, 2), (rows, amount), 0, 4096) + favour
    fixed_rows = jax.random.permutation(jax.random.fold_in(rng, 3), rows)[jnp.arange(amount) % rows]
    tickets = jnp.where(jnp.arange(rows)[:, None] == fixed_rows[None, :], 1 << 14, tickets)
    score = tickets * amount + jnp.arange(amount)
    return lax.top_k(score.astype(jnp.int32), top)[1].astype(jnp.int32)


def assign_block(stream_key, own, number, rows, amount, top, limit, slope):
    ranking = jax.random.permutation(stream_key, amount)
    packed, usual = portions_of(amount, rows * top, limit, slope, True), portions_of(amount, rows * top, limit, slope, False)
    places = jnp.arange(amount)

    def named(tallies, turn):
        used = int((tallies > 0).sum())
        fixed = max(1, used // 4)
        moved = fixed + (places - fixed + turn * (used - fixed)) % max(1, amount - fixed)
        return jnp.zeros((amount,), jnp.int32).at[ranking[jnp.where(places < fixed, places, moved)]].set(jnp.asarray(tallies, jnp.int32))

    tallies = jnp.where(number % 4 == 0, named(packed, number // 4), named(usual, number - number // 4 - 1))
    mixed = jax.random.permutation(jax.random.fold_in(own, 3), amount)
    donor, receiver = mixed[0:amount // 2 * 2:2], mixed[1:amount // 2 * 2:2]
    slack = jnp.minimum(tallies[donor] - 1, limit - tallies[receiver]) // 2
    slack = jnp.where((donor == ranking[0]) | (receiver == ranking[0]) | (tallies[receiver] == 0), 0, jnp.maximum(slack, 0))
    moved = jax.random.randint(jax.random.fold_in(own, 4), (amount // 2,), 0, 1 << 20) % (slack + 1)
    tallies = tallies.at[donor].add(-moved).at[receiver].add(moved)
    items = jnp.searchsorted(jnp.cumsum(tallies), jnp.arange(rows * top), side="right").astype(jnp.int32)
    listing = items.reshape(top, rows).T
    listing = listing[jax.random.permutation(jax.random.fold_in(own, 1), rows)]
    turn = jax.random.randint(jax.random.fold_in(own, 2), (rows, 1), 0, top)
    return jnp.take_along_axis(listing, (jnp.arange(top)[None, :] + turn) % top, axis=1)


def portions_of(amount, total, most, skew, full):
    weights = [(1 << 20) // math.isqrt(rank ** skew) + 1 for rank in range(1, amount + 1)]
    largest = most if full else min(most, max(-(-total // amount), total * weights[0] // sum(weights)))
    least = 1 if total - largest >= amount - 1 else 0
    counts, rest = [largest] + [least] * (amount - 1), total - largest - least * (amount - 1)
    while rest > 0:
        candidates = [i for i in range(1, amount) if counts[i] < largest] or [i for i in range(1, amount) if counts[i] < most]
        pool, budget = sum([weights[i] for i in candidates]), rest
        for i in candidates:
            more = min(most - counts[i], max(1, budget * weights[i] // pool), rest)
            counts[i] = counts[i] + more
            rest = rest - more
    return np.array(counts)


def normal_values(own_key, extent, width, most, cuts=(), kind=jnp.bfloat16):
    array = width * jax.random.normal(own_key, extent, jnp.float32)
    if cuts:
        array = array * levels(own_key, extent, cuts, -0.22, 0.18)
    return jnp.clip(array, -most, most).astype(kind)


def setup_inputs(seed: int = 0) -> dict:
    streams_of = jax.random.split(jax.random.key(seed), 9)
    tokens = normal_values(streams_of[0], (TOKENS, D), 1.0, 6.0, ((0, 256),))
    router_now = normal_values(streams_of[1], (D, EXPERTS), D ** -0.5, 0.078125, ((0, 32),), jnp.float32)
    router_next = normal_values(streams_of[2], (D, EXPERTS), D ** -0.5, 0.078125, ((0, 32),), jnp.float32)
    w_gate = normal_values(streams_of[3], (EXPERTS, D, FF), D ** -0.5, 0.078125, ((0, 8), (2, 32)))
    w_up = normal_values(streams_of[4], (EXPERTS, D, FF), D ** -0.5, 0.078125, ((0, 8), (2, 32)))
    w_down = normal_values(streams_of[5], (EXPERTS, FF, D), FF ** -0.5, 0.0625, ((0, 8), (1, 32)))
    expert_ids_keys = jax.random.split(jax.random.fold_in(streams_of[6], 1), TOKENS // TOK_DEV)
    expert_ids_turns = jax.random.permutation(jax.random.fold_in(streams_of[6], 3), TOKENS // TOK_DEV)
    expert_ids = jax.vmap(lambda own, number: assign_block(jax.random.fold_in(streams_of[6], 2), own, number, TOK_DEV, EXPERTS, TOP, CAP, 2))(expert_ids_keys, expert_ids_turns).reshape((TOKENS, TOP))
    next_ids = picks_of(streams_of[7], TOKENS, EXPERTS, TOP, 2048)
    return dict(tokens=tokens, router_now=router_now, router_next=router_next, w_gate=w_gate, w_up=w_up, w_down=w_down, expert_ids=expert_ids, next_ids=next_ids)


epsilon = 1e-05

def rms_normed(values):
    return values * lax.rsqrt(lax.optimization_barrier(jnp.mean(values * values, axis=-1, keepdims=True)) + epsilon)

def pair_weights(logits, chosen):
    picked = jnp.take_along_axis(logits, chosen, axis=1)
    first = jax.nn.sigmoid(picked[:, 0] - picked[:, 1])
    return jnp.stack([first, 1.0 - first], axis=1)

def reference(tokens, router_now, router_next, w_gate, w_up, w_down, expert_ids, next_ids):
    resid = tokens.astype(jnp.float32)
    normed = rms_normed(resid)
    logits = jnp.dot(normed, router_now, precision=lax.Precision.HIGHEST, preferred_element_type=jnp.float32)
    weights = pair_weights(logits, expert_ids)
    rounded = normed.astype(jnp.bfloat16)
    blocks = TOKENS // TOK_DEV
    flat = expert_ids.reshape(blocks, TOK_DEV * TOP)
    onehot = (flat[:, :, None] == jnp.arange(EXPERTS, dtype=jnp.int32)[None, None, :]).astype(jnp.int32)
    ranks = lax.optimization_barrier(jnp.sum((jnp.cumsum(onehot, axis=1) - onehot) * onehot, axis=2)).reshape(TOKENS, TOP).astype(jnp.int32)
    block_of = jnp.broadcast_to((jnp.arange(TOKENS, dtype=jnp.int32) // TOK_DEV)[:, None], (TOKENS, TOP)).astype(jnp.int32)
    buffer = jnp.zeros((blocks, EXPERTS, CAP, D), jnp.bfloat16)
    buffer = buffer.at[block_of, expert_ids, ranks].set(jnp.broadcast_to(rounded[:, None, :], (TOKENS, TOP, D)))
    rows_in = jnp.transpose(buffer, (1, 0, 2, 3)).reshape(EXPERTS, blocks * CAP, D)

    def expert_out(operands):
        inputs, gate_w, up_w, down_w = operands
        gate = jnp.dot(inputs, gate_w, preferred_element_type=jnp.float32)
        upward = jnp.dot(inputs, up_w, preferred_element_type=jnp.float32)
        hidden = (jax.nn.silu(gate) * upward).astype(jnp.bfloat16)
        return jnp.dot(hidden, down_w, preferred_element_type=jnp.float32)
    outputs = lax.map(expert_out, (rows_in, w_gate, w_up, w_down)).reshape(EXPERTS, blocks, CAP, D)
    picked = outputs[expert_ids, block_of, ranks]
    mixture = lax.optimization_barrier(jnp.sum(picked * weights[:, :, None], axis=1))
    summed = resid + mixture
    layer_out = summed.astype(jnp.bfloat16)
    next_logits = jnp.dot(rms_normed(summed), router_next, precision=lax.Precision.HIGHEST, preferred_element_type=jnp.float32)
    next_weights = pair_weights(next_logits, next_ids)
    return (layer_out, next_logits, next_weights)
```

```python
import jax
import jax.numpy as jnp
import numpy as np
from jax import lax
from jax.sharding import Mesh, PartitionSpec as P

CAP = 4
YH, X, CORES, YL = 2, 4, 2, 2
epsilon = 1e-05
bf16, f32 = jnp.bfloat16, jnp.float32


def rms_normed(values):
    return values * lax.rsqrt(jnp.mean(values * values, axis=-1, keepdims=True) + epsilon)


def pair_weights(logits, chosen):
    picked = jnp.take_along_axis(logits, chosen, axis=1)
    first = jax.nn.sigmoid(picked[:, 0] - picked[:, 1])
    return jnp.stack([first, 1.0 - first], axis=1)


def shift(value, axis, by):
    size = lax.axis_size(axis)
    return lax.ppermute(value, axis, [(i, (i + by) % size) for i in range(size)])


def to_expert(value, dy, dx):
    pairs = [
        (y * X + x, ((y + dy) % YH) * X + (x + dx) % X) for y in range(YH) for x in range(X)
    ]
    return lax.ppermute(value, ("yh", "x"), pairs)


def pair_gather(value, axis):
    other = shift(value, axis, 1)
    low = lax.axis_index(axis) == 0
    return jnp.concatenate([jnp.where(low, value, other), jnp.where(low, other, value)], axis=1)


def whole_routers(router_now, router_next):
    mine = jnp.concatenate([router_now, router_next], axis=1).T
    mine = pair_gather(pair_gather(mine, "c"), "yl")
    zs = lax.axis_size("z")
    per, span = mine.shape[1], 1
    while span < zs:
        mine = jnp.concatenate([mine, shift(mine, "z", -span)], axis=1)
        span *= 2
    start = ((zs - lax.axis_index("z")) % zs) * per
    both = lax.dynamic_slice_in_dim(
        jnp.concatenate([mine, mine], axis=1), start, zs * per, axis=1
    )
    return both


def logits_of(normed, router):
    return lax.dot_general(
        normed,
        router,
        (((1,), (1,)), ((), ())),
        precision=lax.Precision.HIGHEST,
        preferred_element_type=f32,
    )


def on_device(tokens, router_now, router_next, w_gate, w_up, w_down, expert_ids, next_ids):
    tok_count, width = tokens.shape
    top_count = expert_ids.shape[1]
    expert_count = router_now.shape[1]
    slots = expert_count * CAP
    pairs = tok_count * top_count

    weights_in = [(w_gate[0], w_up[0], w_down[0])]
    weights_in.append(tuple(shift(w, "c", 1) for w in weights_in[0]))

    resid = tokens.astype(f32)
    normed = rms_normed(resid)
    rounded = normed.astype(bf16)

    chosen = expert_ids.reshape(pairs)
    onehot = (chosen[:, None] == jnp.arange(expert_count, dtype=jnp.int32)[None, :]).astype(
        jnp.int32
    )
    ranks = jnp.sum((jnp.cumsum(onehot, axis=0) - onehot) * onehot, axis=1)
    dy = (chosen // X - lax.axis_index("yh") + YH) % YH
    dx = (chosen % X - lax.axis_index("x") + X) % X
    places = (dy * X + dx) * CAP + ranks
    place_table = (places[:, None] == jnp.arange(slots, dtype=jnp.int32)[None, :]).astype(f32)
    owners = (
        (jnp.arange(pairs, dtype=jnp.int32) // top_count)[:, None]
        == jnp.arange(tok_count, dtype=jnp.int32)[None, :]
    ).astype(f32)
    sender = jnp.dot(place_table.T, owners, preferred_element_type=f32)
    dispatched = jnp.dot(
        sender.astype(bf16), rounded, preferred_element_type=f32
    ).astype(bf16)

    def block(rows, s):
        return lax.slice_in_dim(rows, s * CAP, (s + 1) * CAP, axis=0)

    moves = [(s // X, s % X) for s in range(expert_count)]
    got = [block(dispatched, 0)] + [
        to_expert(block(dispatched, s), *moves[s]) for s in range(1, expert_count)
    ]
    own = jnp.concatenate(got, axis=0)
    rows0 = jnp.concatenate([own, shift(own, "yl", 1)], axis=0)
    count = rows0.shape[0]
    half = count // 2

    def hidden_of(rows):
        outs = []
        for gate_w, up_w, _ in weights_in:
            gate = jnp.dot(rows, gate_w, preferred_element_type=f32)
            upward = jnp.dot(rows, up_w, preferred_element_type=f32)
            outs.append((jax.nn.silu(gate) * upward).astype(bf16))
        return outs

    reach = lax.axis_size("z") // 2
    ups, downs = [rows0], [rows0]
    for k in range(1, reach):
        ups.append(shift(ups[-1], "z", 1))
        downs.append(shift(downs[-1], "z", -1))
    far = jnp.concatenate(
        [shift(ups[-1][:half], "z", 1), shift(downs[-1][half:], "z", -1)], axis=0
    )

    hid = {}
    h0 = hidden_of(jnp.concatenate([rows0, ups[1], downs[1]], axis=0))
    hid[0], hid[-1], hid[1] = ([h[i * count : (i + 1) * count] for h in h0] for i in range(3))
    for k in range(2, reach):
        hk = hidden_of(jnp.concatenate([ups[k], downs[k]], axis=0))
        hid[-k], hid[k] = ([h[i * count : (i + 1) * count] for h in hk] for i in range(2))
    hid[reach] = hidden_of(far)

    def partial_of(k):
        return sum(
            jnp.dot(h, w[2], preferred_element_type=f32) for h, w in zip(hid[k], weights_in)
        )

    first = partial_of(reach)
    plus = shift(first[:half].astype(bf16), "z", 1)
    minus = shift(first[half:].astype(bf16), "z", -1)
    for k in range(reach - 1, 0, -1):
        a, b = partial_of(k), partial_of(-k)
        if k == reach - 1:
            a = jnp.concatenate([a[:half] + plus.astype(f32), a[half:]], axis=0)
            b = jnp.concatenate([b[:half], b[half:] + minus.astype(f32)], axis=0)
        else:
            a, b = a + plus.astype(f32), b + minus.astype(f32)
        plus = shift(a.astype(bf16), "z", 1)
        minus = shift(b.astype(bf16), "z", -1)
    total = partial_of(0) + plus.astype(f32) + minus.astype(f32)
    theirs = shift(total[half:].astype(bf16), "yl", 1)
    mine = (total[:half] + theirs.astype(f32)).astype(bf16)
    back = [block(mine, 0)] + [
        to_expert(block(mine, s), -moves[s][0], -moves[s][1]) for s in range(1, expert_count)
    ]
    back = jnp.concatenate(back, axis=0)

    routers = whole_routers(router_now, router_next)
    weights = pair_weights(logits_of(normed, routers[:expert_count]), expert_ids)
    combine = jnp.sum(
        (place_table * weights.reshape(pairs)[:, None]).reshape(tok_count, top_count, slots),
        axis=1,
    )
    mixture = jnp.dot(
        combine, back.astype(f32), precision=lax.Precision.HIGHEST, preferred_element_type=f32
    )
    summed = resid + mixture
    layer_out = summed.astype(bf16)
    next_logits = logits_of(rms_normed(summed), routers[expert_count:])
    next_weights = pair_weights(next_logits, next_ids)
    return (layer_out, next_logits, next_weights)


def solution(mesh):
    zs = mesh.devices.size // (YL * CORES * YH * X)
    fine = Mesh(mesh.devices.reshape(zs, YL, CORES, YH, X), ("z", "yl", "c", "yh", "x"))
    dp, expert = ("z", "yl", "c"), ("yh", "x")
    rows = P(dp + expert, None)
    in_specs = (
        rows,
        P(dp, None),
        P(dp, None),
        P(expert, None, dp),
        P(expert, None, dp),
        P(expert, dp, None),
        rows,
        rows,
    )
    return jax.shard_map(
        on_device, mesh=fine, in_specs=in_specs, out_specs=(rows, rows, rows), check_vma=False
    )
```
